128 devices in a mesh: section: 4 (over y), dp: 32 (over x, z, core).
Axes of the slice: x: 4, y: 4, z: 4, core: 2. Of those that a mesh axis runs over, the one named last changes fastest.
Arguments:
- inputs: bfloat16 [4096, 1600], P('dp'), may hold values from -6 to 6
- targets: bfloat16 [4096, 1600], P('dp'), may hold values from -6 to 6
- weight_in: bfloat16 [4, 1600, 3200], P('section'), may hold values from -0.15625 to 0.15625
- hidden_bias: float32 [4, 3200], P('section'), may hold values from -3 to 3
- norm_gain: float32 [4, 1600], P('section'), may hold values from 0.5 to 1.5
- weight_out: bfloat16 [4, 3200, 1600], P('section'), may hold values from -0.109375 to 0.109375
- current: float32 [4, 3200, 1600], P('section', 'dp')
- previous: float32 [4, 3200, 1600], P('section', 'dp')
- older_basis: float32 [2, 4, 3200, 1600], P(None, 'section', 'dp')
- beta_before: float32 [1], replicated, may hold values from 1 to 4
Outputs:
- next_vector: float32 [4, 3200, 1600], P('section', 'dp')
- tridiagonal_entries: float32 [2], replicated
The draws below stay inside these ranges and needn't reach their ends.
All inputs are finite; a program needn't handle non-finite values.
Results may differ from the reference program's by a relative error of at most 0.012.
Values may be sent and summed in bfloat16 or wider, within the bound.
A program may use at most 192 MiB of HBM per device.

```python
import math
from functools import partial
import jax
import jax.numpy as jnp
from jax import lax

D = 1600
FF = 3200
KEEP = 2
SECTIONS = 4
ROWS = 4096


def spread_vectors(key, members):
    subkeys = jax.random.split(key, 4)
    normal_part = jax.random.normal(subkeys[0], (members, SECTIONS, FF, D), jnp.float32)
    rise_along = jnp.exp(jnp.log(3.0) * jnp.arange(FF, dtype=jnp.float32) / FF)[:, None]
    section_scale = jnp.exp(jnp.log(2.0) * jax.random.uniform(subkeys[3], (members, SECTIONS, 1, 1), jnp.float32))
    return normal_part * rise_along * section_scale


def lanczos_vectors(key):
    raw_draw = spread_vectors(jax.random.fold_in(key, 7), KEEP + 2)
    members = []
    for member in range(KEEP + 2):
        vector = raw_draw[member]
        for passes in range(2):
            for earlier in members:
                vector = vector - jnp.mean(vector * earlier) * earlier
        vector = vector / jnp.sqrt(jnp.mean(vector * vector))
        members.append(vector)
    correlation = jax.random.uniform(jax.random.fold_in(key, 8), (KEEP,), jnp.float32, 0.3, 0.6)
    drifted = members[KEEP]
    for member in range(KEEP):
        drifted = drifted + correlation[member] * members[member]
    drifted = drifted / jnp.sqrt(jnp.mean(drifted * drifted))
    return (jnp.stack(members[:KEEP]), drifted, members[KEEP + 1])


def draw_current(key, part):
    return lanczos_vectors(key)[2]


def draw_previous(key, part):
    return lanczos_vectors(key)[1]


def draw_older_basis(key, part):
    return lanczos_vectors(key)[0]


def block_scale(own_key, extent, pieces, least, top_value):
    level, own = 1.0, jax.random.fold_in(own_key, 6)
    for axis_at, shards_of in pieces:
        heights = jnp.exp(jax.random.uniform(jax.random.fold_in(own, axis_at), (shards_of,), jnp.float32, least / len(pieces), top_value / len(pieces)))
        level = level * jnp.repeat(heights, extent[axis_at] // shards_of).reshape([-1 if axis == axis_at else 1 for axis in range(len(extent))])
    return level


def noise(rng, dims, deviation, limit, cuts=(), held_as=jnp.bfloat16):
    drawn = jax.random.normal(rng, dims, jnp.float32) * deviation
    if len(cuts) > 0:
        drawn = block_scale(rng, dims, cuts, -0.22, 0.18) * drawn
    return jnp.clip(drawn, min=-limit, max=limit).astype(held_as)


def setup_inputs(seed: int = 0) -> dict:
    key_of = jax.random.split(jax.random.key(seed), 11)
    return {
        "inputs": noise(key_of[0], (ROWS, D), 1.0, 6.0, ((0, 32),)),
        "targets": noise(key_of[1], (ROWS, D), 1.0, 6.0, ((0, 32),)),
        "weight_in": noise(key_of[2], (SECTIONS, D, FF), D ** -0.5, 0.15625, ((0, 4),)),
        "hidden_bias": noise(key_of[3], (SECTIONS, FF), 0.5, 3.0, ((0, 4),), jnp.float32),
        "norm_gain": jnp.clip(1.0 + 0.1 * jax.random.normal(key_of[4], (SECTIONS, D), jnp.float32), 0.5, 1.5),
        "weight_out": noise(key_of[5], (SECTIONS, FF, D), FF ** -0.5, 0.109375, ((0, 4),)),
        "current": draw_current(jax.random.fold_in(key_of[10], 71), 0),
        "previous": draw_previous(jax.random.fold_in(key_of[10], 71), 0),
        "older_basis": draw_older_basis(jax.random.fold_in(key_of[10], 71), 0),
        "beta_before": jnp.clip(jnp.exp(jax.random.uniform(key_of[9], (1,), jnp.float32, math.log(1.0), math.log(4.0))), 1.0, 4.0),
    }


def gelu_tanh(values):
    return jax.nn.gelu(values, approximate=True)

def gelu_slope(values):
    return jax.jvp(gelu_tanh, (values,), (jnp.ones_like(values),))[1]

def gelu_bend(values):
    return jax.jvp(gelu_slope, (values,), (jnp.ones_like(values),))[1]

def normalize(values, gain_row):
    mean_value = lax.optimization_barrier(jnp.mean(values, axis=-1, keepdims=True))
    centered = values - mean_value
    variance = lax.optimization_barrier(jnp.mean(centered * centered, axis=-1, keepdims=True))
    return centered * lax.rsqrt(variance + 1e-05) * gain_row

def times_transposed(left, right):
    return lax.dot_general(left, right, (((1,), (1,)), ((), ())), preferred_element_type=jnp.float32)

def contract_rows(left, right):
    return lax.dot_general(left, right, (((0,), (0,)), ((), ())), preferred_element_type=jnp.float32)

def layer_inner(rows_in, tangent_in, weight_in, bias_row, gain_row):
    rows_float = rows_in.astype(jnp.float32)
    tangent_float = tangent_in.astype(jnp.float32)
    normed, normed_dot = jax.jvp(partial(normalize, gain_row=gain_row), (rows_float,), (tangent_float,))
    preact = jnp.dot(normed.astype(jnp.bfloat16), weight_in, preferred_element_type=jnp.float32) + bias_row
    preact_dot = jnp.dot(normed_dot.astype(jnp.bfloat16), weight_in, preferred_element_type=jnp.float32)
    hidden = gelu_tanh(preact).astype(jnp.bfloat16)
    hidden_dot = (gelu_slope(preact) * preact_dot).astype(jnp.bfloat16)
    return (rows_float, tangent_float, preact, preact_dot, hidden, hidden_dot)

def layer_forward(rows_in, tangent_in, weight_in, bias_row, gain_row, weight_out, direction):
    rows_float, tangent_float, preact, preact_dot, hidden, hidden_dot = layer_inner(rows_in, tangent_in, weight_in, bias_row, gain_row)
    rows_out = rows_float + jnp.dot(hidden, weight_out, preferred_element_type=jnp.float32)
    tangent_out = tangent_float + jnp.dot(hidden_dot, weight_out, preferred_element_type=jnp.float32)
    tangent_out = tangent_out + jnp.dot(hidden, direction, preferred_element_type=jnp.float32)
    return (rows_out.astype(jnp.bfloat16), tangent_out.astype(jnp.bfloat16))

def layer_backward(rows_in, tangent_in, grad_out, grad_dot_out, weight_in, bias_row, gain_row, weight_out, direction):
    rows_float, tangent_float, preact, preact_dot, hidden, hidden_dot = layer_inner(rows_in, tangent_in, weight_in, bias_row, gain_row)
    back_hidden = times_transposed(grad_out, weight_out)
    back_hidden_dot = times_transposed(grad_dot_out, weight_out) + times_transposed(grad_out, direction)
    slope = gelu_slope(preact)
    pre_grad = (slope * back_hidden).astype(jnp.bfloat16)
    pre_grad_dot = (gelu_bend(preact) * preact_dot * back_hidden + slope * back_hidden_dot).astype(jnp.bfloat16)
    norm_grad = times_transposed(pre_grad, weight_in)
    norm_grad_dot = times_transposed(pre_grad_dot, weight_in)

    def pull_back(values, cotangent):
        return jax.vjp(partial(normalize, gain_row=gain_row), values)[1](cotangent)[0]
    grad_in, grad_in_dot = jax.jvp(pull_back, (rows_float, norm_grad), (tangent_float, norm_grad_dot))
    grad_next = (grad_out.astype(jnp.float32) + grad_in).astype(jnp.bfloat16)
    grad_dot_next = (grad_dot_out.astype(jnp.float32) + grad_in_dot).astype(jnp.bfloat16)
    return (grad_next, grad_dot_next, hidden, hidden_dot)

def reference(inputs, targets, weight_in, hidden_bias, norm_gain, weight_out, current, previous, older_basis, beta_before):
    levels = weight_in.shape[0]
    row_count = float(inputs.shape[0])
    rows_now = inputs
    tangent_now = jnp.zeros_like(inputs)
    saved = []
    for level in range(levels):
        direction = current[level].astype(jnp.bfloat16)
        saved.append((rows_now, tangent_now))
        rows_now, tangent_now = layer_forward(rows_now, tangent_now, weight_in[level], hidden_bias[level], norm_gain[level], weight_out[level], direction)
    grad_now = ((rows_now.astype(jnp.float32) - targets.astype(jnp.float32)) / row_count).astype(jnp.bfloat16)
    grad_dot_now = (tangent_now.astype(jnp.float32) / row_count).astype(jnp.bfloat16)
    products = [None] * levels
    for level in reversed(range(levels)):
        direction = current[level].astype(jnp.bfloat16)
        grad_next, grad_dot_next, hidden, hidden_dot = layer_backward(saved[level][0], saved[level][1], grad_now, grad_dot_now, weight_in[level], hidden_bias[level], norm_gain[level], weight_out[level], direction)
        products[level] = contract_rows(hidden_dot, grad_now) + contract_rows(hidden, grad_dot_now)
        grad_now, grad_dot_now = (grad_next, grad_dot_next)
    hvp = jnp.stack(products)
    entry_count = float(hvp.size)
    start_vec = hvp - beta_before[0] * previous
    alpha_value = jnp.sum(start_vec * current) / entry_count
    first_resid = start_vec - alpha_value * current
    basis = jnp.concatenate([older_basis, previous[None], current[None]], axis=0)
    coeffs = lax.optimization_barrier(jnp.sum(basis * first_resid[None], axis=(1, 2, 3))) / entry_count
    second = first_resid - lax.optimization_barrier(jnp.sum(coeffs[:, None, None, None] * basis, axis=0))
    beta_value = jnp.sqrt(jnp.sum(second * second) / entry_count + 1e-06)
    return (second / beta_value, jnp.stack([alpha_value, beta_value]))
```

```python
import functools

import jax
import jax.numpy as jnp
from jax import lax
from jax.experimental import pallas as pl
from jax.experimental.pallas import tpu as pltpu
from jax.sharding import PartitionSpec as P

MESH = pl.DeviceIdType.MESH
F32 = jnp.float32
BF16 = jnp.bfloat16

T = 128
D = 1600
FF = 3200
CH = 640
NCH = FF // CH
SH = 100
WIN = 112
CUT = 64
TOKENS = 4096.0
ENTRIES = 20480000.0
GC = 0.7978845608028654
GA = 0.044715


def dot(a, b):
    return jnp.dot(a, b, preferred_element_type=F32)


def dot_t(a, b):
    return lax.dot_general(a, b, (((1,), (1,)), ((), ())), preferred_element_type=F32)


def row_mean(v):
    return jnp.mean(v, axis=1, keepdims=True)


def total(v):
    return jnp.sum(jnp.sum(v, axis=0, keepdims=True), axis=1, keepdims=True)


def mult(v, n):
    return v if isinstance(v, int) else pl.multiple_of(v, n)


def loop(n, fn):
    def step(i, carry):
        fn(i)
        return carry

    lax.fori_loop(0, n, step, 0)


def kernel(
    x_hbm, t_hbm, wi_hbm, bias_hbm, gain_hbm, wo_hbm, cur_hbm, prev_hbm, old_hbm, beta_ref,
    out_ref, tri_ref,
    wi, wo, g, bias, gain, xb, tb, gg, pg, one, two, nb,
    slope, bend, pd, bk, hid, hdot, ht, l0, lp, lr, r1, r2,
    xhat, xdot, acc, mg, ag, rs, rd, pm,
    cur, prev, old, gr, tile, tile2, ar1, ar2,
    lsem, wsem, gsem, hsem, ssem, ysem, yrem, csem, crem, r1sem, r2sem, rss, a1s, a1r, a2s, a2r,
):
    goal = two
    hw = xdot.at[pl.ds(0, WIN)]
    hv = mg.at[pl.ds(0, SH)]
    s = lax.axis_index("section")
    me = lax.axis_index("dp")
    c = lax.rem(me, 2)
    x = me // 8
    z = lax.rem(me // 2, 4)
    p = x * (1 - c) + z * c
    q = z * (1 - c) + x * c

    def m4(v):
        return lax.rem(v + 8, 4)

    def dev_of(pp, qq, cc):
        xx = pp * (1 - cc) + qq * cc
        zz = qq * (1 - cc) + pp * cc
        return (xx * 4 + zz) * 2 + cc

    def dev(pp, qq):
        return dev_of(m4(pp), m4(qq), c)

    partner = me + 1 - 2 * c

    def remote(src, dst, send, recv, sec, dp):
        return pltpu.make_async_remote_copy(
            src_ref=src, dst_ref=dst, send_sem=send, recv_sem=recv,
            device_id=(sec, dp), device_id_type=MESH,
        )

    loads = [
        pltpu.make_async_copy(cur_hbm, cur, lsem.at[0]),
        pltpu.make_async_copy(bias_hbm, bias, lsem.at[1]),
        pltpu.make_async_copy(gain_hbm, gain, lsem.at[2]),
        pltpu.make_async_copy(t_hbm, goal, lsem.at[3]),
        pltpu.make_async_copy(prev_hbm, prev, lsem.at[4]),
        pltpu.make_async_copy(old_hbm, old, lsem.at[5]),
    ]
    x_load = pltpu.make_async_copy(x_hbm, xb, lsem.at[6])
    loads[0].start()

    @pl.when(s == 0)
    def _():
        x_load.start()

    loads[1].start()
    loads[2].start()

    def wi_load(j):
        cols = pl.ds(mult(j * CH, 128), CH)
        return pltpu.make_async_copy(wi_hbm.at[:, cols], wi.at[:, cols], wsem.at[2 * j])

    def wo_load(j):
        cols = pl.ds(mult(j * CH, 128), CH)
        return pltpu.make_async_copy(wo_hbm.at[:, cols], wo.at[:, cols], wsem.at[2 * j + 1])

    for j in range(NCH):
        wi_load(j).start()
        wo_load(j).start()
    for one_load in loads[4:]:
        one_load.start()

    @pl.when(s == 3)
    def _():
        loads[3].start()

    barrier = pltpu.get_barrier_semaphore()

    def greet_section(i, _):
        sec = lax.rem(s + i // 2, 4)
        dp = me + lax.rem(i, 2) * (1 - 2 * c)
        pl.semaphore_signal(barrier, inc=1, device_id=(sec, dp), device_id_type=MESH)
        return _

    def greet_plane(i, _):
        dp = lax.rem(me + 2 * i, 32)
        pl.semaphore_signal(barrier, inc=1, device_id=(s, dp), device_id_type=MESH)
        return _

    lax.fori_loop(1, 8, greet_section, 0)
    lax.fori_loop(1, 16, greet_plane, 0)

    loads[0].wait()
    hw[...] = jnp.zeros((WIN, D), F32)
    for k in range(4):

        @pl.when(lax.rem(me, 4) == k)
        def _(k=k):
            hw[4 * k:4 * k + SH, :] = cur[...]

    def win(d):
        return g.at[pl.ds(mult(d * WIN, 16), WIN)]

    def win_part(d, half):
        if half == 0:
            return g.at[pl.ds(mult(d * WIN, 16), CUT)]
        return g.at[pl.ds(mult(d * WIN + CUT, 16), WIN - CUT)]

    g[pl.ds(mult(me * WIN, 16), WIN), :] = hw[...].astype(BF16)
    pl.semaphore_wait(barrier, 22)

    a_up, a_down, b_up, b_down = dev(p + 1, q), dev(p - 1, q), dev(p, q + 1), dev(p, q - 1)
    far = dev(p + 2, q)
    w_b = [dev(p, q - 1), dev(p - 1, q - 1), dev(p + 1, q - 1), dev(p + 2, q - 1)]
    w_u = [dev(p, q + 1), dev(p - 1, q + 1), dev(p + 1, q + 1), dev(p + 2, q + 1)]
    w_f = [dev(p, q + 2), dev(p - 1, q + 2), dev(p + 1, q + 2), dev(p + 2, q + 2)]

    first_steps = [
        ([(a_down, None)], [(a_down, 0, a_up), (a_down, None, b_up), (a_down, None, b_down), (a_down, None, partner)]),
        ([(a_up, None)], [(a_up, 1, a_down), (a_up, None, b_up), (a_up, None, b_down), (a_up, None, partner)]),
        ([(w_b[0], None)], [(w_b[0], None, b_up), (w_b[0], None, partner)]),
        ([(w_u[0], None)], [(w_u[0], None, partner)]),
        ([(far, 0), (far, 1)], [(far, None, b_up), (far, None, b_down), (far, None, partner)]),
    ]
    rest_steps = [
        ([(w_b[1], None)], [(w_b[1], None, b_up), (w_b[1], None, partner)]),
        ([(w_u[2], None)], [(w_u[2], None, b_down), (w_u[2], None, partner)]),
        ([(w_u[1], None)], [(w_u[1], None, partner)]),
        ([(w_b[2], None)], [(w_b[2], None, partner)]),
        ([(w_u[3], None)], [(w_u[3], None, b_down), (w_u[3], None, partner)]),
    ]
    rest_steps += [([(d, None)], [(d, None, partner)]) for d in [w_b[3]] + w_f]
    own_sends = [(me, None, to) for to in (a_up, a_down, b_up, b_down, partner)]
    plan = own_sends + [send for _, sent in first_steps + rest_steps for send in sent]

    def share(i):
        d, part, to = plan[i]
        if part is None:
            return remote(win(d), win(d), ssem.at[i], gsem.at[d], s, to)
        return remote(win_part(d, part), win_part(d, part), ssem.at[i], hsem.at[part], s, to)

    def got(d, part=None):
        if part is None:
            remote(win(d), win(d), ssem.at[0], gsem.at[d], s, partner).wait_recv()
        else:
            ref = win_part(d, part)
            remote(ref, ref, ssem.at[0], hsem.at[part], s, partner).wait_recv()

    def run_steps(steps, at):
        for waits, sent in steps:
            for d, part in waits:
                got(d, part)
            for _ in sent:
                share(at).start()
                at += 1
        return at

    rest_at = len(own_sends) + sum(len(sent) for _, sent in first_steps)
    for i in range(len(own_sends)):
        share(i).start()

    def gather_first():
        run_steps(first_steps, len(own_sends))

    def gather_rest():
        run_steps(rest_steps, rest_at)

        def other(k):
            got(2 * k + 1 - c)

        loop(16, other)
        for i in range(len(plan)):
            share(i).wait_send()

        def pack(i):
            src = mult(i * (4 * WIN), 16)
            dst = mult(i * (4 * SH), 16)
            for k in range(4):
                value = g[pl.ds(src + k * WIN, WIN), :]
                at = dst + k * 96
                if k == 0:
                    g[pl.ds(at, WIN), :] = value
                else:
                    edge = g[pl.ds(at, 16), :].astype(F32) + value[:16].astype(F32)
                    g[pl.ds(at, 16), :] = edge.astype(BF16)
                    g[pl.ds(at + 16, WIN - 16), :] = value[16:]

        loop(8, pack)

    def hop(k):
        src = (one, two, one, two)[k]
        dst = (xb, tb, gg.at[pl.ds(0, T)], gg.at[pl.ds(T, T)])[k]
        to = lax.rem(s + (1 if k < 2 else 3), 4)
        return remote(src, dst, ysem.at[k], yrem.at[k], to, me)

    def cols(j):
        return pl.ds(mult(j * CH, 128), CH)

    def rows(j):
        return pl.ds(mult(j * CH, 16), CH)

    def forward():
        @pl.when(s == 0)
        def _():
            x_load.wait()

        loads[1].wait()
        loads[2].wait()

        @pl.when(s > 0)
        def _():
            hop(0).wait_recv()

        rows_in = xb[...].astype(F32)
        centered = rows_in - row_mean(rows_in)
        r = lax.rsqrt(row_mean(centered * centered) + 1e-05)
        hat = centered * r
        rs[...] = r
        xhat[...] = hat
        nb[...] = (hat * gain[...]).astype(BF16)
        acc[...] = jnp.zeros((T, D), F32)

        def chunk(j):
            wi_load(j).wait()
            wo_load(j).wait()
            v = dot(nb[...], wi[:, cols(j)]) + bias[:, cols(j)]
            v2 = v * v
            t = jnp.tanh(GC * (v + GA * (v * v2)))
            h = (0.5 * v * (1.0 + t)).astype(BF16)
            hid[:, cols(j)] = h
            acc[...] += dot_t(h, wo[:, cols(j)])
            up = GC * (1.0 + (3.0 * GA) * v2)
            om = 1.0 - t * t
            slope[:, cols(j)] = 0.5 * (1.0 + t) + 0.5 * v * om * up
            bend[:, cols(j)] = om * (up + 0.5 * v * ((6.0 * GC * GA) * v - 2.0 * t * up * up))

        loop(NCH, chunk)
        one[...] = (xb[...].astype(F32) + acc[...]).astype(BF16)

        @pl.when(s < 3)
        def _():
            hop(0).start()

        @pl.when(s == 3)
        def _():
            loads[3].wait()
            gg[0:T, :] = ((one[...].astype(F32) - goal[...].astype(F32)) * (1.0 / TOKENS)).astype(BF16)

    def gather_and_forward(k):
        @pl.when(k == 1)
        def _():
            gather_first()

        @pl.when(k == 2)
        def _():
            gather_rest()

        @pl.when(k == jnp.minimum(s, 2))
        def _():
            forward()

    loop(3, gather_and_forward)

    @pl.when(s < 3)
    def _():
        hop(0).wait_send()

    def swap(k):
        src = (lp, gg.at[pl.ds(0, T)], gg.at[pl.ds(T, T)])[k]
        dst = (lr, pg.at[pl.ds(0, T)], pg.at[pl.ds(T, T)])[k]
        return remote(src, dst, csem.at[k], crem.at[k], s, partner)

    def tangent():
        acc[...] = jnp.zeros((T, D), F32)

        def early(j):
            acc[...] += dot(hid[:, cols(j)], g[rows(j), :])

        loop(NCH, early)

        @pl.when(s > 0)
        def _():
            hop(1).wait_recv()
            tan = tb[...].astype(F32)
            moved = tan - row_mean(tan)
            hat = xhat[...]
            r = rs[...]
            along = row_mean(hat * moved)
            hat_dot = r * (moved - hat * along)
            rd[...] = -(r * r) * along
            xdot[...] = hat_dot
            nb[...] = (hat_dot * gain[...]).astype(BF16)

            def chunk(j):
                v = dot(nb[...], wi[:, cols(j)])
                pd[:, cols(j)] = v
                h = (slope[:, cols(j)] * v).astype(BF16)
                hdot[:, cols(j)] = h
                acc[...] += dot_t(h, wo[:, cols(j)])

            loop(NCH, chunk)
            two[...] = (tb[...].astype(F32) + acc[...]).astype(BF16)

        @pl.when(s == 0)
        def _():
            two[...] = acc[...].astype(BF16)

        @pl.when(s < 3)
        def _():
            hop(1).start()

        @pl.when(s == 3)
        def _():
            gg[T:2 * T, :] = (two[...].astype(F32) * (1.0 / TOKENS)).astype(BF16)

        @pl.when(s == 0)
        def _():
            ht[:, 0:T] = jnp.zeros((FF, T), BF16)

        def turn(j):
            ht[rows(j), T:2 * T] = hid[:, cols(j)].astype(F32).T.astype(BF16)

            @pl.when(s > 0)
            def _():
                ht[rows(j), 0:T] = hdot[:, cols(j)].astype(F32).T.astype(BF16)

        loop(NCH, turn)

        def line_up(i):
            e, a = i // 4, lax.rem(i, 4)
            to = pl.ds(mult(i * WIN, 16), WIN)
            shift = (e == 0) * 2 + (e == 1) * 1 + (e == 2) * 3
            mine = dev_of(a, m4(q + shift), c)
            theirs = dev_of(a, m4(p + shift), 1 - c)
            l0[to, :] = ht[pl.ds(mult(mine * SH - 4 * lax.rem(mine, 4), 16), WIN), :]
            lp[to, :] = ht[pl.ds(mult(theirs * SH - 4 * lax.rem(theirs, 4), 16), WIN), :]

        loop(16, line_up)
        swap(0).start()

    def backward():
        @pl.when(s < 3)
        def _():
            hop(2).wait_recv()

        swap(1).start()

        @pl.when(s > 0)
        def _():
            acc[...] = jnp.zeros((T, D), F32)

            def chunk(j):
                v = dot(gg[0:T, :], wo[:, cols(j)])
                bk[:, cols(j)] = v
                pre = (slope[:, cols(j)] * v).astype(BF16)
                acc[...] += dot_t(pre, wi[:, cols(j)])

            loop(NCH, chunk)
            m = acc[...] * gain[...]
            hat = xhat[...]
            p_mean = row_mean(m * hat)
            a = m - row_mean(m) - hat * p_mean
            mg[...] = m
            ag[...] = a
            pm[...] = p_mean
            one[...] = (gg[0:T, :].astype(F32) + rs[...] * a).astype(BF16)
            hop(2).start()

    def tangent_and_backward(k):
        @pl.when(k == 1)
        def _():
            tangent()

        @pl.when(k == jnp.where(s == 3, 0, 2))
        def _():
            backward()

    loop(3, tangent_and_backward)

    @pl.when(s < 3)
    def _():
        hop(1).wait_send()

    @pl.when(s > 0)
    def _():
        def chunk(j):
            v = dot_t(gg[0:T, :], g[rows(j), :])
            bk[:, cols(j)] = bend[:, cols(j)] * pd[:, cols(j)] * bk[:, cols(j)] + slope[:, cols(j)] * v

        loop(NCH, chunk)

    lane = lax.broadcasted_iota(jnp.int32, (8, 128), 1)
    loads[4].wait()
    loads[5].wait()

    def member(i):
        return (old[0], old[1], prev[...], cur[...])[i]

    grams = jnp.zeros((8, 128), F32)
    for i in range(4):
        for j in range(i, 4):
            grams = jnp.where(lane == 5 * i + j, total(member(i) * member(j)), grams)
    gr[...] = grams

    @pl.when(s < 3)
    def _():
        hop(3).wait_recv()

    swap(2).start()

    @pl.when(s > 0)
    def _():
        acc[...] = jnp.zeros((T, D), F32)

        def chunk(j):
            v = dot(gg[T:2 * T, :], wo[:, cols(j)])
            pre = (bk[:, cols(j)] + slope[:, cols(j)] * v).astype(BF16)
            acc[...] += dot_t(pre, wi[:, cols(j)])

        loop(NCH, chunk)
        m_dot = acc[...] * gain[...]
        hat = xhat[...]
        hat_dot = xdot[...]
        p_dot = row_mean(m_dot * hat) + row_mean(mg[...] * hat_dot)
        a_dot = m_dot - row_mean(m_dot) - hat_dot * pm[...] - hat * p_dot
        moved = rd[...] * ag[...] + rs[...] * a_dot
        two[...] = (gg[T:2 * T, :].astype(F32) + moved).astype(BF16)
        hop(3).start()

    for k in range(3):
        swap(k).wait_recv()

    def slots(i, n):
        return pl.ds(i * WIN, n * WIN)

    def rs_copy(k):
        src = g.at[(slots(0, 2), slots(2, 2), slots(6, 2), slots(4, 2), slots(8, 2), slots(10, 2))[k]]
        dst = r1.at[(slots(0, 2), slots(6, 2), slots(4, 2), slots(2, 2), slots(8, 2), slots(10, 2))[k]]
        to = (b_up, b_down, b_up, b_up, b_down, b_down)[k]
        return remote(src, dst, rss.at[k], r1sem.at[k], s, to)

    def piece(e):
        at = pl.ds(mult(e * (4 * WIN), 16), 4 * WIN)
        left = jnp.concatenate([l0[at, :], lr[at, :]], axis=1)
        for lo, hi in ((0, 512), (512, 1024), (1024, D)):
            right = jnp.concatenate([gg[:, lo:hi], pg[:, lo:hi]], axis=0)
            g[at, lo:hi] = dot(left, right).astype(BF16)

        @pl.when(e == 0)
        def _():
            rs_copy(0).start()
            rs_copy(1).start()

        @pl.when(e == 1)
        def _():
            rs_copy(2).start()

        @pl.when(e == 2)
        def _():
            rs_copy(4).start()

    loop(4, piece)

    def add_into(at, other, n):
        g[at, :] = (g[at, :].astype(F32) + other[...].astype(F32)).astype(BF16)

    rs_copy(0).wait_recv()
    add_into(slots(4, 2), r1.at[slots(0, 2)], 2)
    rs_copy(3).start()
    rs_copy(1).wait_recv()
    add_into(slots(10, 2), r1.at[slots(6, 2)], 2)
    rs_copy(5).start()
    for k in (2, 4, 3, 5):
        rs_copy(k).wait_recv()

    def own_slot(a):
        return mult((12 + a) * WIN, 16)

    def summed(a):
        v = g[pl.ds(own_slot(a), WIN), :].astype(F32)
        v += r1[pl.ds(mult((2 + a) * WIN, 16), WIN), :].astype(F32)
        v += r1[pl.ds(mult((8 + a) * WIN, 16), WIN), :].astype(F32)
        return v

    tail = WIN - CUT

    def part(a, half):
        if half == 0:
            return pl.ds(own_slot(a), CUT)
        return pl.ds(mult(own_slot(a) + CUT, 16), tail)

    a_far, a_next, a_last = m4(p + 2), m4(p + 1), m4(p - 1)

    def rs2_copy(k):
        src = (part(a_far, 0), part(a_far, 1), part(a_next, 1), part(a_next, 0), part(a_last, 0), part(a_last, 1))[k]
        dst = (
            pl.ds(0, CUT), pl.ds(CUT, tail), pl.ds(WIN + CUT, tail), pl.ds(WIN, CUT),
            pl.ds(2 * WIN, CUT), pl.ds(2 * WIN + CUT, tail),
        )[k]
        to = (a_up, a_down, a_up, a_up, a_down, a_down)[k]
        return remote(g.at[src], r2.at[dst], rss.at[6 + k], r2sem.at[k], s, to)

    g[pl.ds(own_slot(a_far), WIN), :] = summed(a_far).astype(BF16)
    rs2_copy(0).start()
    rs2_copy(1).start()
    g[pl.ds(own_slot(a_next), WIN), :] = summed(a_next).astype(BF16)
    rs2_copy(2).start()
    g[pl.ds(own_slot(a_last), WIN), :] = summed(a_last).astype(BF16)
    rs2_copy(4).start()
    hw[...] = summed(p)
    rs2_copy(0).wait_recv()
    add_into(part(a_next, 0), r2.at[pl.ds(0, CUT)], 1)
    rs2_copy(3).start()
    rs2_copy(1).wait_recv()
    add_into(part(a_last, 1), r2.at[pl.ds(CUT, tail)], 1)
    rs2_copy(5).start()
    for k in (2, 4, 3, 5):
        rs2_copy(k).wait_recv()
    hw[...] += r2[WIN:2 * WIN, :].astype(F32) + r2[2 * WIN:3 * WIN, :].astype(F32)
    for k in range(4):

        @pl.when(lax.rem(me, 4) == k)
        def _(k=k):
            hv[...] = hw[4 * k:4 * k + SH, :]

    grams = gr[...]
    for i in range(4):
        grams = jnp.where(lane == 5 * i + 4, total(member(i) * hv[...]), grams)
    grams = jnp.where(lane == 24, total(hv[...] * hv[...]), grams)
    tile[...] = grams

    mine1 = s * 2 + c

    def a1_copy(i):
        sec = lax.rem(s + i // 2, 4)
        dp = me + lax.rem(i, 2) * (1 - 2 * c)
        return remote(tile, ar1.at[mine1], a1s.at[i], a1r.at[mine1], sec, dp)

    def a1_wait(i):
        them = lax.rem(s + i // 2, 4) * 2 + lax.rem(c + i, 2)
        remote(tile, ar1.at[them], a1s.at[i], a1r.at[them], s, partner).wait_recv()

    def span(lo, hi, fn):
        def step(i, carry):
            fn(i)
            return carry

        lax.fori_loop(lo, hi, step, 0)

    span(1, 8, lambda i: a1_copy(i).start())
    ar1[mine1] = grams
    span(1, 8, a1_wait)
    level = ar1[0]
    for i in range(1, 8):
        level = level + ar1[i]
    tile2[...] = level
    mine2 = me // 2

    def a2_copy(i):
        dp = lax.rem(me + 2 * i, 32)
        return remote(tile2, ar2.at[mine2], a2s.at[i], a2r.at[mine2], s, dp)

    def a2_wait(i):
        them = lax.rem(mine2 + i, 16)
        remote(tile2, ar2.at[them], a2s.at[i], a2r.at[them], s, partner).wait_recv()

    span(1, 16, lambda i: a2_copy(i).start())
    ar2[mine2] = level
    span(1, 16, a2_wait)
    level = ar2[0]
    for i in range(1, 16):
        level = level + ar2[i]
    level = level[0:1, :] * (1.0 / ENTRIES)
    lane1 = lane[0:1, :]

    def entry(i, j):
        i, j = min(i, j), max(i, j)
        return jnp.sum(jnp.where(lane1 == 5 * i + j, level, 0.0), axis=1, keepdims=True)

    gram = [[entry(i, j) for j in range(5)] for i in range(4)]
    square = entry(4, 4)
    start = jnp.full((1, 1), -beta_ref[0], F32)
    alpha = gram[3][4] + start * gram[2][3]
    first = [None, None, start, -alpha]
    weights = []
    for j in range(4):
        coeff = gram[j][4] + start * gram[2][j] - alpha * gram[3][j]
        weights.append(-coeff if first[j] is None else first[j] - coeff)
    norm = square
    for i in range(4):
        norm = norm + 2.0 * weights[i] * gram[i][4]
        for j in range(4):
            norm = norm + weights[i] * gram[i][j] * weights[j]
    beta = jnp.sqrt(jnp.maximum(norm, 0.0) + 1e-06)
    second = hv[...]
    for j in range(4):
        second = second + weights[j] * member(j)
    out_ref[...] = second / beta
    tri_ref[...] = jnp.where(lane == 0, alpha, jnp.where(lane == 1, beta, 0.0))

    for k in range(3):
        swap(k).wait_send()

    @pl.when(s > 0)
    def _():
        hop(2).wait_send()
        hop(3).wait_send()

    for k in range(6):
        rs_copy(k).wait_send()
        rs2_copy(k).wait_send()
    span(1, 8, lambda i: a1_copy(i).wait_send())
    span(1, 16, lambda i: a2_copy(i).wait_send())


def body(inputs, targets, weight_in, hidden_bias, norm_gain, weight_out, current, previous, older_basis, beta_before):
    any_spec = pl.BlockSpec(memory_space=pl.ANY)
    vmem = pltpu.VMEM
    dma = pltpu.SemaphoreType.DMA
    scratch = [
        vmem((D, FF), BF16),
        vmem((D, FF), BF16),
        vmem((32 * WIN, D), BF16),
        vmem((1, FF), F32),
        vmem((1, D), F32),
        vmem((T, D), BF16),
        vmem((T, D), BF16),
        vmem((2 * T, D), BF16),
        vmem((2 * T, D), BF16),
        vmem((T, D), BF16),
        vmem((T, D), BF16),
        vmem((T, D), BF16),
        vmem((T, FF), F32),
        vmem((T, FF), F32),
        vmem((T, FF), F32),
        vmem((T, FF), F32),
        vmem((T, FF), BF16),
        vmem((T, FF), BF16),
        vmem((FF, 2 * T), BF16),
        vmem((16 * WIN, 2 * T), BF16),
        vmem((16 * WIN, 2 * T), BF16),
        vmem((16 * WIN, 2 * T), BF16),
        vmem((12 * WIN, D), BF16),
        vmem((3 * WIN, D), BF16),
        vmem((T, D), F32),
        vmem((T, D), F32),
        vmem((T, D), F32),
        vmem((T, D), F32),
        vmem((T, D), F32),
        vmem((T, 1), F32),
        vmem((T, 1), F32),
        vmem((T, 1), F32),
        vmem((SH, D), F32),
        vmem((SH, D), F32),
        vmem((2, SH, D), F32),
        vmem((8, 128), F32),
        vmem((8, 128), F32),
        vmem((8, 128), F32),
        vmem((8, 8, 128), F32),
        vmem((16, 8, 128), F32),
        dma((7,)),
        dma((2 * NCH,)),
        dma((32,)),
        dma((2,)),
        dma((34,)),
        dma((4,)),
        dma((4,)),
        dma((3,)),
        dma((3,)),
        dma((6,)),
        dma((6,)),
        dma((12,)),
        dma((8,)),
        dma((8,)),
        dma((16,)),
        dma((16,)),
    ]
    out, tri = pl.pallas_call(
        kernel,
        out_shape=(
            jax.ShapeDtypeStruct((SH, D), F32),
            jax.ShapeDtypeStruct((8, 128), F32),
        ),
        in_specs=[any_spec] * 9 + [pl.BlockSpec(memory_space=pltpu.SMEM)],
        out_specs=(pl.BlockSpec(memory_space=pltpu.VMEM), pl.BlockSpec(memory_space=pltpu.VMEM)),
        scratch_shapes=scratch,
        compiler_params=pltpu.CompilerParams(
            collective_id=0, has_side_effects=True, vmem_limit_bytes=67043328
        ),
    )(
        inputs, targets, weight_in[0], hidden_bias, norm_gain, weight_out[0].T,
        current[0], previous[0], older_basis[:, 0], beta_before,
    )
    return out[None], tri[0, :2]


def solution(mesh):
    dp = "dp"
    in_specs = (
        P(dp, None),
        P(dp, None),
        P("section", None, None),
        P("section", None),
        P("section", None),
        P("section", None, None),
        P("section", dp, None),
        P("section", dp, None),
        P(None, "section", dp, None),
        P(),
    )
    out_specs = (P("section", dp, None), P())
    return jax.shard_map(body, mesh=mesh, in_specs=in_specs, out_specs=out_specs, check_vma=False)
```
